128 devices in a mesh: north: 32 (over z, x, core), deep: 4 (over y).
Axes of the slice: x: 4, y: 4, z: 4, core: 2. Of those that a mesh axis runs over, the one named last changes fastest.
Arguments:
- source: float32 [512, 512, 2048], P(None, 'north', 'deep'), may hold values from -6 to 6
- symbol_x: float32 [512], replicated, may hold values from 0.3 to 3
- symbol_y: float32 [512], replicated, may hold values from 0.3 to 3
- symbol_z: float32 [2048], replicated, may hold values from 0.3 to 3
Outputs:
- coefficients: float32 [256, 256, 1024], P('north', 'deep')
The draws below stay inside these ranges and needn't reach their ends.
All inputs are finite; a program needn't handle non-finite values.
Results may differ from the reference program's by a relative error of at most 0.000071.
Values sent between devices are 32-bit elements; how exact they have to be, the bound alone decides.
A program may use at most 128 MiB of HBM per device.

```python
import jax
import jax.numpy as jnp
from jax import lax

GRID_X = 512
GRID_Y = 512
GRID_Z = 2048


def block_levels(stream_key, shape, shards, least, largest):
    gain = 1.0
    for dim, parts in shards:
        heights = jax.random.uniform(jax.random.fold_in(jax.random.fold_in(stream_key, 6), dim), (parts,), jnp.float32, least / len(shards), largest / len(shards))
        gain = gain * jnp.repeat(jnp.exp(heights), shape[dim] // parts).reshape((-1,) + (1,) * (len(shape) - 1 - dim))
    return gain


def noise(rng, shape, scale, most, shards=(), dtype=jnp.bfloat16):
    level = block_levels(rng, shape, shards, -0.22, 0.18) if shards else 1.0
    entries = jax.random.normal(rng, shape, jnp.float32) * scale * level
    return jnp.minimum(jnp.maximum(entries, -most), most).astype(dtype)


def setup_inputs(seed: int = 0) -> dict:
    arg_keys = jax.random.split(jax.random.key(seed), 5)
    source = noise(arg_keys[0], (GRID_X, GRID_Y, GRID_Z), 1.0, 6.0, ((1, 32), (2, 4)), jnp.float32)
    symbol_x = jnp.clip(jax.random.uniform(arg_keys[1], (GRID_X,), jnp.float32, 0.3, 3.0), 0.3, 3.0)
    symbol_y = jnp.clip(jax.random.uniform(arg_keys[2], (GRID_Y,), jnp.float32, 0.3, 3.0), 0.3, 3.0)
    symbol_z = jnp.clip(jax.random.uniform(arg_keys[3], (GRID_Z,), jnp.float32, 0.3, 3.0), 0.3, 3.0)
    return {"source": source, "symbol_x": symbol_x, "symbol_y": symbol_y, "symbol_z": symbol_z}


def basis_table(count):
    rank = jnp.arange(count)
    angle = jnp.pi / (count + 1) * ((rank[:, None] + 1) * (rank[None, :] + 1) % (2 * count + 2)).astype(jnp.float32)
    return jnp.sin(angle) * (2.0 / (count + 1)) ** 0.5

def along_dim(values, dim):
    moved = jnp.tensordot(values, basis_table(values.shape[dim]), axes=([dim], [0]), precision=lax.Precision.HIGHEST)
    return jnp.moveaxis(moved, -1, dim)

def reference(source, symbol_x, symbol_y, symbol_z):
    coefficients = source
    coefficients = along_dim(coefficients, 0)
    coefficients = lax.slice_in_dim(coefficients, 0, GRID_X // 2, axis=0)
    coefficients = along_dim(coefficients, 1)
    coefficients = lax.slice_in_dim(coefficients, 0, GRID_Y // 2, axis=1)
    coefficients = along_dim(coefficients, 2)
    coefficients = lax.slice_in_dim(coefficients, 0, GRID_Z // 2, axis=2)
    symbol = symbol_x[:GRID_X // 2][:, None, None] + symbol_y[:GRID_Y // 2][None, :, None] + symbol_z[:GRID_Z // 2][None, None, :]
    coefficients = coefficients * lax.rsqrt(symbol)
    return coefficients
```

```python
import functools

import jax
import jax.numpy as jnp
import numpy as np
from jax import lax
from jax.experimental import pallas as pl
from jax.experimental.pallas import tpu as pltpu
from jax.sharding import PartitionSpec as P

NORTH, DEEP = 32, 4
MESH = pl.DeviceIdType.MESH
F32, BF16 = jnp.float32, jnp.bfloat16


def split(values):
    high = values.astype(BF16)
    return high, (values - high.astype(F32)).astype(BF16)


def dot3(a_high, a_low, b_high, b_low):
    dot = functools.partial(jnp.dot, preferred_element_type=F32)
    return dot(a_high, b_high) + dot(a_low, b_high) + dot(a_high, b_low)


def peer_order():
    far = [0, 1, 2, 1]
    offsets = [(a, b, c) for a in range(4) for b in range(4) for c in range(2)]
    offsets.remove((0, 0, 0))
    return sorted(offsets, key=lambda o: (-(far[o[0]] + far[o[1]]), o[2], o[0], o[1]))


def kernel(
    source, table_high, table_low, fine, coarse, sym_x, sym_y, sym_z, out,
    planes, first, gath_a, gath_b, half_a, recv_a, half_b, recv_b, last_b, out_a,
    z_high, z_low, left_high, left_low, col_y,
    load_sem, na_send, na_recv, y1_send, y1_recv, y2_send, y2_recv,
    nb_send, nb_recv, y3_send, y3_recv, put_sem,
):
    n = lax.axis_index("north")
    d = lax.axis_index("deep")
    z_pos, x_pos, core = n // 8, (n // 2) % 4, n % 2

    def peer(offset):
        a, b, c = offset
        return ((z_pos + a) % 4) * 8 + ((x_pos + b) % 4) * 2 + (core + c) % 2

    barrier = pltpu.get_barrier_semaphore()
    for offset in peer_order():
        pl.semaphore_signal(barrier, inc=1, device_id=(peer(offset), d), device_id_type=MESH)
    for e in range(1, DEEP):
        pl.semaphore_signal(barrier, inc=1, device_id=(n, (d + e) % 4), device_id_type=MESH)

    def load(y):
        return pltpu.make_async_copy(source.at[:, y, :], planes.at[y], load_sem.at[y])

    for y in range(16):
        load(y).start()

    def wait_bytes(ref, sem):
        pltpu.make_async_copy(ref, ref, sem).wait()

    flat = first.reshape(4 * 256 * 16, 128)

    def x_step(y, _):
        load(y).wait()
        for half in range(2):
            high, low = split(planes[y, :, half * 256 : half * 256 + 256])
            res = dot3(table_high[...], table_low[...], high, low)
            for c in range(2):
                for m in range(NORTH):
                    row = (half * 2 + c) * 4096 + m * 128
                    flat[pl.ds(row + y, 8, stride=16), :] = res[
                        m * 8 : m * 8 + 8, c * 128 : c * 128 + 128
                    ]
        return 0

    lax.fori_loop(0, 16, x_step, 0)

    pl.semaphore_wait(barrier, NORTH - 1 + DEEP - 1)

    modes = first.reshape(4, 8, 4, 8, 16, 128)

    for s in range(4):
        g = (n + s) % 4
        for e in range(1, DEEP):
            to = (d + e) % 4
            pltpu.make_async_remote_copy(
                modes.at[:, :, g, 4 + to],
                gath_b.at[s, d],
                y1_send,
                y1_recv.at[s],
                device_id=(n, to),
                device_id_type=MESH,
            ).start()
        for offset in peer_order():
            to = peer(offset)
            pltpu.make_async_remote_copy(
                first.at[s, pl.ds(8 * to, 4)],
                gath_a.at[s, :, pl.ds(16 * n, 16)],
                na_send,
                na_recv.at[s],
                device_id=(to, d),
                device_id_type=MESH,
            ).start()

    for s in range(4):
        g = (n + s) % 4
        gath_a[s, :, pl.ds(16 * n, 16)] = first[s, pl.ds(8 * n, 4)]
        gath_b[s, d] = modes[:, :, g, 4 + d]

    fine_sin, fine_cos = fine.at[0], fine.at[1]

    def table_step(p, _):
        for q in range(2):
            cols = slice(q * 512, q * 512 + 512)
            sin_p = coarse[0, pl.ds(p, 1), cols]
            cos_p = coarse[1, pl.ds(p, 1), cols]

            def rows_step(r, _):
                rows = pl.ds(pl.multiple_of(r * 16, 16), 16)
                values = sin_p * fine_cos[rows, cols] + cos_p * fine_sin[rows, cols]
                high, low = split(values)
                to = pl.ds(pl.multiple_of(p * 128 + r * 16, 16), 16)
                z_high[to, cols] = high
                z_low[to, cols] = low
                return 0

            lax.fori_loop(0, 8, rows_step, 0)
        return 0

    lax.fori_loop(0, 16, table_step, 0)

    row_id = lax.broadcasted_iota(jnp.int32, (128, 128), 0)
    col_id = lax.broadcasted_iota(jnp.int32, (128, 128), 1)
    for h in range(2):
        picked = jnp.where(row_id == col_id, sym_y[0:1, h * 128 : h * 128 + 128], 0.0)
        col_y[h * 128 : h * 128 + 128, :] = jnp.broadcast_to(
            jnp.sum(picked, axis=1, keepdims=True), (128, 128)
        )

    def z_stage(load_block, rows, store):
        for b in range(16):
            high, low = split(load_block(b))
            left_high[0:rows, b * 128 : b * 128 + 128] = high
            left_low[0:rows, b * 128 : b * 128 + 128] = low

        def col_step(t, _):
            cols = pl.ds(pl.multiple_of(t * 256, 256), 256)
            res = dot3(
                left_high[0:rows, :], left_low[0:rows, :], z_high[:, cols], z_low[:, cols]
            )
            store(t, cols, res)
            return 0

        lax.fori_loop(0, 4, col_step, 0)

    def send_half_b(s, h):
        g = (n + s) % 4
        for r in range(8):
            mem = (n // 4 + 4 + r) % 8
            to = 4 * mem + g

            @pl.when(to != n)
            def _():
                pltpu.make_async_remote_copy(
                    half_b.at[h, s, mem],
                    recv_b.at[h, pl.ds(16 * n, 16)],
                    nb_send,
                    nb_recv.at[h],
                    device_id=(to, d),
                    device_id_type=MESH,
                ).start()

    def middle_step(s, _):
        wait_bytes(gath_a.at[s, :, pl.ds(0, 496)], na_recv.at[s])
        for pair in range(2):
            high, low = split(
                jnp.concatenate([gath_a[s, 2 * pair], gath_a[s, 2 * pair + 1]], axis=1)
            )
            res = dot3(table_high[...], table_low[...], high, low)
            half_a[s, 2 * pair] = res[:, :128]
            half_a[s, 2 * pair + 1] = res[:, 128:]
        for e in range(1, DEEP):
            to = (d + e) % 4
            pltpu.make_async_remote_copy(
                half_a.at[s, :, pl.ds(64 * to, 64)],
                recv_a.at[d, s],
                y2_send,
                y2_recv,
                device_id=(n, to),
                device_id_type=MESH,
            ).start()
        recv_a[d, s] = half_a[s, :, pl.ds(64 * d, 64)]

        wait_bytes(gath_b.at[s, pl.ds(0, 3)], y1_recv.at[s])

        def store(t, cols, res):
            half_b[t // 2, s, :, :, pl.ds(pl.multiple_of((t % 2) * 256, 256), 256)] = (
                res.reshape(8, 16, 256)
            )

        z_stage(lambda b: gath_b[s, b // 4, b % 4].reshape(128, 128), 128, store)
        send_half_b(s, 0)
        return 0

    lax.fori_loop(0, 4, middle_step, 0)
    lax.fori_loop(0, 4, lambda s, c: (send_half_b(s, 1), c)[1], 0)

    for h in range(2):
        recv_b[h, pl.ds(16 * n, 16)] = half_b[h, 0, n // 4]

    def half_step(h, _):
        wait_bytes(recv_b.at[h, pl.ds(0, 496)], nb_recv.at[h])
        for q in range(2):
            cols = slice(q * 256, q * 256 + 256)
            high, low = split(recv_b[h, :, cols])
            res = dot3(table_high[...], table_low[...], high, low)
            at = pl.ds(pl.multiple_of(h * 512 + q * 256, 256), 256)
            symbol = (sym_x[8 * n + 4 + d] + col_y[:, 0:1]) + sym_z[0:1, at]
            last_b[h, :, cols] = res * lax.rsqrt(symbol)
        for e in range(1, DEEP):
            to = (d + e) % 4
            pltpu.make_async_remote_copy(
                last_b.at[h, pl.ds(64 * to, 64)],
                out.at[4 + d, :, pl.ds(pl.multiple_of(h * 512, 512), 512)],
                y3_send,
                y3_recv,
                device_id=(n, to),
                device_id_type=MESH,
            ).start()
        put_b(h).start()
        return 0

    def put_b(h):
        return pltpu.make_async_copy(
            last_b.at[h, pl.ds(64 * d, 64)],
            out.at[4 + d, :, pl.ds(pl.multiple_of(h * 512, 512), 512)],
            put_sem.at[h],
        )

    lax.fori_loop(0, 2, half_step, 0)

    wait_bytes(recv_a.at[pl.ds(0, 3)], y2_recv)

    def store_a(t, cols, res):
        for i in range(4):
            symbol = (sym_x[8 * n + i] + col_y[pl.ds(64 * d, 64), 0:1]) + sym_z[0:1, cols]
            out_a[i, :, cols] = res[i * 64 : i * 64 + 64] * lax.rsqrt(symbol)

    z_stage(lambda b: recv_a[b // 4, b % 4].reshape(256, 128), 256, store_a)
    put_a = pltpu.make_async_copy(out_a, out.at[pl.ds(0, 4)], put_sem.at[2])
    put_a.start()

    wait_bytes(first.at[:, pl.ds(0, 124)], na_send)
    wait_bytes(gath_b.at[:, pl.ds(0, 3)], y1_send)
    wait_bytes(recv_a.at[pl.ds(0, 3)], y2_send)
    wait_bytes(recv_b.at[:, pl.ds(0, 496)], nb_send)
    wait_bytes(last_b.at[:, pl.ds(0, 192)], y3_send)
    for h in range(2):
        put_b(h).wait()
    put_a.wait()
    wait_bytes(last_b.at[:, pl.ds(0, 192)], y3_recv)


def tables():
    count = 512
    rank = np.arange(count, dtype=np.int64)
    angle = np.pi / (count + 1) * (((rank[:256, None] + 1) * (rank[None, :] + 1)) % (2 * count + 2))
    table = np.sin(angle) * np.sqrt(2.0 / (count + 1))
    table = table.astype(np.float32)
    high = table.astype(BF16)
    low = (table - high.astype(np.float32)).astype(BF16)
    count = 2048
    rank = np.arange(1024, dtype=np.int64)[None, :] + 1
    step = np.pi / (count + 1)
    fine = step * ((np.arange(128, dtype=np.int64)[:, None] * rank) % (2 * count + 2))
    coarse = step * (((128 * np.arange(16, dtype=np.int64)[:, None] + 1) * rank) % (2 * count + 2))
    gain = np.sqrt(2.0 / (count + 1))
    fine = np.stack([np.sin(fine), np.cos(fine)]).astype(np.float32)
    coarse = (gain * np.stack([np.sin(coarse), np.cos(coarse)])).astype(np.float32)
    return high, low, fine, coarse


def on_device(source, symbol_x, symbol_y, symbol_z):
    high, low, fine, coarse = tables()
    vmem = pl.BlockSpec(memory_space=pltpu.VMEM)
    anywhere = pl.BlockSpec(memory_space=pl.ANY)
    dma = pltpu.SemaphoreType.DMA
    return pl.pallas_call(
        kernel,
        out_shape=jax.ShapeDtypeStruct((8, 64, 1024), F32),
        in_specs=[anywhere, vmem, vmem, vmem, vmem]
        + [pl.BlockSpec(memory_space=pltpu.SMEM), vmem, vmem],
        out_specs=anywhere,
        scratch_shapes=[
            pltpu.VMEM((16, 512, 512), F32),
            pltpu.VMEM((4, 256, 16, 128), F32),
            pltpu.VMEM((4, 4, 512, 128), F32),
            pltpu.VMEM((4, 4, 4, 8, 16, 128), F32),
            pltpu.VMEM((4, 4, 256, 128), F32),
            pltpu.VMEM((4, 4, 4, 64, 128), F32),
            pltpu.VMEM((2, 4, 8, 16, 512), F32),
            pltpu.VMEM((2, 512, 512), F32),
            pltpu.VMEM((2, 256, 512), F32),
            pltpu.VMEM((4, 64, 1024), F32),
            pltpu.VMEM((2048, 1024), BF16),
            pltpu.VMEM((2048, 1024), BF16),
            pltpu.VMEM((256, 2048), BF16),
            pltpu.VMEM((256, 2048), BF16),
            pltpu.VMEM((256, 128), F32),
            dma((16,)),
            dma,
            dma((4,)),
            dma,
            dma((4,)),
            dma,
            dma,
            dma,
            dma((2,)),
            dma,
            dma,
            dma((3,)),
        ],
        compiler_params=pltpu.CompilerParams(
            collective_id=0, has_side_effects=True, vmem_limit_bytes=63 << 20
        ),
    )(
        source,
        high,
        low,
        fine,
        coarse,
        symbol_x,
        symbol_y.reshape(1, 512),
        symbol_z.reshape(1, 2048),
    )


def solution(mesh):
    in_specs = (P(None, "north", "deep"), P(), P(), P())
    out_specs = P("north", "deep", None)
    return jax.shard_map(
        on_device, mesh=mesh, in_specs=in_specs, out_specs=out_specs, check_vma=False
    )
```

```python
import functools

import jax
import jax.numpy as jnp
import numpy as np
from jax import lax
from jax.experimental import pallas as pl
from jax.experimental.pallas import tpu as pltpu
from jax.sharding import PartitionSpec as P

NORTH, DEEP = 32, 4
CHUNKS, WIDE = 4, 2
MESH = pl.DeviceIdType.MESH
F32, BF16 = jnp.float32, jnp.bfloat16


def split(values):
    high = values.astype(BF16)
    return high, (values - high.astype(F32)).astype(BF16)


def dot3(a_high, a_low, b_high, b_low):
    dot = functools.partial(jnp.dot, preferred_element_type=F32)
    return dot(a_high, b_high) + dot(a_low, b_high) + dot(a_high, b_low)


def peer_order():
    far = [0, 1, 2, 1]
    offsets = [(a, b, c) for a in range(4) for b in range(4) for c in range(2)]
    offsets.remove((0, 0, 0))
    return sorted(offsets, key=lambda o: (-(far[o[0]] + far[o[1]]), o[2], o[0], o[1]))


def wait_bytes(ref, sem):
    pltpu.make_async_copy(ref, ref, sem).wait()


def kernel(
    source, x_hbm, y_hbm, fine_hbm, coarse_hbm, sym_x_hbm, sym_y_hbm, sym_z_hbm, out,
    planes, x_tab, y_tab, fine, coarse, sym_x, sym_y, sym_z, first_a, first_b, gath_a, gath_b, half_a, recv_a,
    half_b, recv_b, last_b, z_high, z_low, left_high, left_low, col_y,
    load_sem, tab_sem, na_send, na_recv, y1_send, y1_recv, y2_send, y2_recv,
    nb_send, nb_recv, y3_send, y3_recv,
):
    n = lax.axis_index("north")
    d = lax.axis_index("deep")
    z_pos, x_pos, core = n // 8, (n // 2) % 4, n % 2

    def place(offset):
        a, b, c = offset
        return (z_pos + a) % 4, (x_pos + b) % 4, (core + c) % 2

    def peer(offset):
        a, b, c = place(offset)
        return a * 8 + b * 2 + c

    barrier = pltpu.get_barrier_semaphore()
    for offset in peer_order():
        pl.semaphore_signal(barrier, inc=1, device_id=(peer(offset), d), device_id_type=MESH)
    for e in range(1, DEEP):
        pl.semaphore_signal(barrier, inc=1, device_id=(n, (d + e) % 4), device_id_type=MESH)

    tabs = [
        pltpu.make_async_copy(a, b, tab_sem.at[i])
        for i, (a, b) in enumerate(
            [
                (x_hbm, x_tab),
                (y_hbm, y_tab),
                (fine_hbm, fine),
                (coarse_hbm, coarse),
                (sym_x_hbm, sym_x),
                (sym_y_hbm, sym_y),
                (sym_z_hbm, sym_z),
            ]
        )
    ]

    def load(y):
        return pltpu.make_async_copy(source.at[:, y, :], planes.at[y], load_sem.at[y])

    tabs[0].start()
    for y in range(16):
        load(y).start()
    for tab in tabs[1:]:
        tab.start()
    tabs[0].wait()

    flat_a = first_a.reshape(4 * 128 * 16, 128)

    def x_step(pair, _):
        for j in range(2):
            load(2 * pair + j).wait()
        for j in range(2):
            y = 2 * pair + j
            for half in range(2):
                high, low = split(planes[y, :, half * 256 : half * 256 + 256])
                res = dot3(x_tab[0], x_tab[1], high, low)
                for c in range(2):
                    cols = slice(c * 128, c * 128 + 128)
                    zc = half * 2 + c
                    for m in range(16):
                        row = (zc * 128 + m * 8) * 16
                        flat_a[pl.ds(row + y, 8, stride=16), :] = res[m * 8 : m * 8 + 8, cols]
                    first_b[zc, y] = res[128:, cols].reshape(4, 32, 128)
        return 0

    def send_first_b(q, _):
        for e in range(1, DEEP):
            to = (d + e) % 4
            pltpu.make_async_remote_copy(
                first_b.at[:, pl.ds(4 * q, 4), to],
                gath_b.at[q, d],
                y1_send,
                y1_recv.at[q],
                device_id=(n, to),
                device_id_type=MESH,
            ).start()
        return 0

    lax.fori_loop(0, 6, x_step, 0)
    pl.semaphore_wait(barrier, NORTH - 1 + DEEP - 1)
    lax.fori_loop(0, 3, send_first_b, 0)
    lax.fori_loop(6, 8, x_step, 0)
    send_first_b(3, 0)

    def send_a(s, _):
        for offset in peer_order():
            to = peer(offset)
            pltpu.make_async_remote_copy(
                first_a.at[s, pl.ds(4 * to, 4)],
                gath_a.at[s, :, pl.ds(16 * n, 16)],
                na_send,
                na_recv.at[s],
                device_id=(to, d),
                device_id_type=MESH,
            ).start()
        return 0

    lax.fori_loop(0, 4, send_a, 0)

    for s in range(4):
        gath_a[s, :, pl.ds(16 * n, 16)] = first_a[s, pl.ds(4 * n, 4)]
        gath_b[s, d] = first_b[:, pl.ds(4 * s, 4), d]

    for tab in tabs[1:]:
        tab.wait()

    def table_step(p, _):
        for q in range(2):
            cols = slice(q * 512, q * 512 + 512)
            sin_p = coarse[0, pl.ds(p, 1), cols]
            cos_p = coarse[1, pl.ds(p, 1), cols]

            def rows_step(r, _):
                rows = pl.ds(pl.multiple_of(r * 16, 16), 16)
                values = sin_p * fine[1, rows, cols] + cos_p * fine[0, rows, cols]
                high, low = split(values)
                to = pl.ds(pl.multiple_of(p * 128 + r * 16, 16), 16)
                z_high[to, cols] = high
                z_low[to, cols] = low
                return 0

            lax.fori_loop(0, 8, rows_step, 0)
        return 0

    lax.fori_loop(0, 16, table_step, 0)

    row_id = lax.broadcasted_iota(jnp.int32, (128, 128), 0)
    col_id = lax.broadcasted_iota(jnp.int32, (128, 128), 1)
    for h in range(2):
        picked = jnp.where(row_id == col_id, sym_y[0:1, h * 128 : h * 128 + 128], 0.0)
        col_y[h * 128 : h * 128 + 128, :] = jnp.broadcast_to(
            jnp.sum(picked, axis=1, keepdims=True), (128, 128)
        )

    def z_stage(load_block, rows, store):
        for b in range(16):
            high, low = split(load_block(b))
            left_high[0:rows, b * 128 : b * 128 + 128] = high
            left_low[0:rows, b * 128 : b * 128 + 128] = low

        def col_step(t, _):
            cols = pl.ds(pl.multiple_of(t * 256, 256), 256)
            res = dot3(
                left_high[0:rows, :], left_low[0:rows, :], z_high[:, cols], z_low[:, cols]
            )
            store(t, cols, res)
            return 0

        lax.fori_loop(0, 4, col_step, 0)

    def step_a(s):
        wait_bytes(gath_a.at[s, :, pl.ds(0, 496)], na_recv.at[s])
        for i in range(0, 4, 2):
            high, low = split(jnp.concatenate([gath_a[s, i], gath_a[s, i + 1]], axis=1))
            res = dot3(y_tab[0], y_tab[1], high, low)
            half_a[s, i] = res[:, :128]
            half_a[s, i + 1] = res[:, 128:]
        for e in range(1, DEEP):
            to = (d + e) % 4
            pltpu.make_async_remote_copy(
                half_a.at[s, :, pl.ds(64 * to, 64)],
                recv_a.at[d, s],
                y2_send,
                y2_recv,
                device_id=(n, to),
                device_id_type=MESH,
            ).start()
        recv_a[d, s] = half_a[s, :, pl.ds(64 * d, 64)]

    flat_b = half_b.reshape(8 * 32 * 16, 128)

    def step_b(q):
        wait_bytes(gath_b.at[q, pl.ds(0, 3)], y1_recv.at[q])

        def store(t, cols, res):
            for c in range(2):
                for y in range(4):
                    for m in range(4):
                        at = y * 32 + m * 8
                        row = ((2 * t + c) * 32 + m * 8) * 16 + 4 * q + y
                        flat_b[pl.ds(row, 8, stride=16), :] = res[
                            at : at + 8, c * 128 : c * 128 + 128
                        ]

        z_stage(lambda b: gath_b[q, b // 4, b % 4].reshape(128, 128), 128, store)

    def middle_step(s, _):
        step_b(s)
        step_a(s)
        return 0

    lax.fori_loop(0, 3, middle_step, 0)
    step_b(3)

    def send_b(ch, _):
        for offset in peer_order():
            to = peer(offset)
            pltpu.make_async_remote_copy(
                half_b.at[pl.ds(WIDE * ch, WIDE), to],
                recv_b.at[pl.ds(WIDE * ch, WIDE), pl.ds(16 * n, 16)],
                nb_send,
                nb_recv.at[ch],
                device_id=(to, d),
                device_id_type=MESH,
            ).start()
        return 0

    lax.fori_loop(0, CHUNKS, send_b, 0)
    recv_b[:, pl.ds(16 * n, 16)] = half_b[:, n]
    step_a(3)

    def last_step(ch, _):
        wait_bytes(recv_b.at[pl.ds(WIDE * ch, WIDE), pl.ds(0, 496)], nb_recv.at[ch])
        cols = pl.ds(pl.multiple_of(ch * WIDE * 128, WIDE * 128), WIDE * 128)
        high, low = split(jnp.concatenate([recv_b[WIDE * ch + j] for j in range(WIDE)], axis=1))
        res = dot3(y_tab[0], y_tab[1], high, low)
        symbol = (sym_x[8 * n + 4 + d] + col_y[:, 0:1]) + sym_z[0:1, cols]
        last_b[:, cols] = res * lax.rsqrt(symbol)
        for e in range(1, DEEP):
            to = (d + e) % 4
            pltpu.make_async_remote_copy(
                last_b.at[pl.ds(64 * to, 64), cols],
                out.at[4 + d, :, cols],
                y3_send,
                y3_recv,
                device_id=(n, to),
                device_id_type=MESH,
            ).start()
        out[4 + d, :, cols] = last_b[pl.ds(64 * d, 64), cols]
        return 0

    lax.fori_loop(0, CHUNKS, last_step, 0)

    wait_bytes(recv_a.at[pl.ds(0, 3)], y2_recv)

    def store_a(t, cols, res):
        for i in range(4):
            symbol = (sym_x[8 * n + i] + col_y[pl.ds(64 * d, 64), 0:1]) + sym_z[0:1, cols]
            out[i, :, cols] = res[i * 64 : i * 64 + 64] * lax.rsqrt(symbol)

    z_stage(lambda b: recv_a[b // 4, b % 4].reshape(256, 128), 256, store_a)

    wait_bytes(first_a.at[:, pl.ds(0, 124)], na_send)
    wait_bytes(gath_b.at[:, pl.ds(0, 3)], y1_send)
    wait_bytes(recv_a.at[pl.ds(0, 3)], y2_send)
    wait_bytes(half_b.at[:, pl.ds(0, 31)], nb_send)
    wait_bytes(last_b.at[pl.ds(0, 192)], y3_send)
    wait_bytes(last_b.at[pl.ds(0, 192)], y3_recv)


def halves(table):
    table = table.astype(np.float32)
    high = table.astype(BF16)
    return np.stack([high, (table - high.astype(np.float32)).astype(BF16)])


def tables():
    count = 512
    rank = np.arange(count, dtype=np.int64)
    angle = np.pi / (count + 1) * (((rank[:256, None] + 1) * (rank[None, :] + 1)) % (2 * count + 2))
    table = np.sin(angle) * np.sqrt(2.0 / (count + 1))
    rows = [8 * n + i for n in range(NORTH) for i in range(4)]
    rows += [8 * n + 4 + e for e in range(DEEP) for n in range(NORTH)]
    count = 2048
    rank = np.arange(1024, dtype=np.int64)[None, :] + 1
    step = np.pi / (count + 1)
    fine = step * ((np.arange(128, dtype=np.int64)[:, None] * rank) % (2 * count + 2))
    coarse = step * (((128 * np.arange(16, dtype=np.int64)[:, None] + 1) * rank) % (2 * count + 2))
    gain = np.sqrt(2.0 / (count + 1))
    fine = np.stack([np.sin(fine), np.cos(fine)]).astype(np.float32)
    coarse = (gain * np.stack([np.sin(coarse), np.cos(coarse)])).astype(np.float32)
    return halves(table[rows]), halves(table), fine, coarse


def on_device(source, symbol_x, symbol_y, symbol_z):
    vmem = pl.BlockSpec(memory_space=pltpu.VMEM)
    anywhere = pl.BlockSpec(memory_space=pl.ANY)
    dma = pltpu.SemaphoreType.DMA
    return pl.pallas_call(
        kernel,
        out_shape=pltpu.VMEM((8, 64, 1024), F32),
        in_specs=[anywhere] * 8,
        out_specs=vmem,
        scratch_shapes=[
            pltpu.VMEM((16, 512, 512), F32),
            pltpu.VMEM((2, 256, 512), BF16),
            pltpu.VMEM((2, 256, 512), BF16),
            pltpu.VMEM((2, 128, 1024), F32),
            pltpu.VMEM((2, 16, 1024), F32),
            pltpu.SMEM((512,), F32),
            pltpu.VMEM((1, 512), F32),
            pltpu.VMEM((1, 2048), F32),
            pltpu.VMEM((4, 128, 16, 128), F32),
            pltpu.VMEM((4, 16, 4, 32, 128), F32),
            pltpu.VMEM((4, 4, 512, 128), F32),
            pltpu.VMEM((4, 4, 4, 4, 32, 128), F32),
            pltpu.VMEM((4, 4, 256, 128), F32),
            pltpu.VMEM((4, 4, 4, 64, 128), F32),
            pltpu.VMEM((8, 32, 16, 128), F32),
            pltpu.VMEM((8, 512, 128), F32),
            pltpu.VMEM((256, 1024), F32),
            pltpu.VMEM((2048, 1024), BF16),
            pltpu.VMEM((2048, 1024), BF16),
            pltpu.VMEM((256, 2048), BF16),
            pltpu.VMEM((256, 2048), BF16),
            pltpu.VMEM((256, 128), F32),
            dma((16,)),
            dma((7,)),
            dma,
            dma((4,)),
            dma,
            dma((4,)),
            dma,
            dma,
            dma,
            dma((CHUNKS,)),
            dma,
            dma,
        ],
        compiler_params=pltpu.CompilerParams(
            collective_id=0, has_side_effects=True, vmem_limit_bytes=60 << 20
        ),
    )(
        source,
        *tables(),
        symbol_x,
        symbol_y.reshape(1, 512),
        symbol_z.reshape(1, 2048),
    )


def solution(mesh):
    in_specs = (P(None, "north", "deep"), P(), P(), P())
    out_specs = P("north", "deep", None)
    return jax.shard_map(
        on_device, mesh=mesh, in_specs=in_specs, out_specs=out_specs, check_vma=False
    )
```

```python
import functools

import jax
import jax.numpy as jnp
import numpy as np
from jax import lax
from jax.experimental import pallas as pl
from jax.experimental.pallas import tpu as pltpu
from jax.sharding import PartitionSpec as P

NORTH, DEEP = 32, 4
CHUNKS, WIDE = 4, 2
MESH = pl.DeviceIdType.MESH
F32, BF16 = jnp.float32, jnp.bfloat16


def split(values):
    high = values.astype(BF16)
    return high, (values - high.astype(F32)).astype(BF16)


def dot3(a_high, a_low, b_high, b_low):
    dot = functools.partial(jnp.dot, preferred_element_type=F32)
    return dot(a_high, b_high) + dot(a_low, b_high) + dot(a_high, b_low)


def peer_order():
    far = [0, 1, 2, 1]
    offsets = [(a, b, c) for a in range(4) for b in range(4) for c in range(2)]
    offsets.remove((0, 0, 0))
    return sorted(offsets, key=lambda o: (-(far[o[0]] + far[o[1]]), o[2], o[0], o[1]))


def wait_bytes(ref, sem):
    pltpu.make_async_copy(ref, ref, sem).wait()


def kernel(
    source, x_hbm, y_hbm, fine_hbm, coarse_hbm, sym_x_hbm, sym_y_hbm, sym_z_hbm, out,
    planes, x_tab, y_tab, fine, coarse, sym_x, sym_y, sym_z, first_a, first_b, gath_a, gath_b, half_a, recv_a,
    half_b, recv_b, last_b, z_high, z_low, left_high, left_low, col_y,
    load_sem, tab_sem, na_send, na_recv, y1_send, y1_recv, y2_send, y2_recv,
    nb_send, nb_recv, y3_send, y3_recv, heard,
):
    n = lax.axis_index("north")
    d = lax.axis_index("deep")
    z_pos, x_pos, core = n // 8, (n // 2) % 4, n % 2

    def place(offset):
        a, b, c = offset
        return (z_pos + a) % 4, (x_pos + b) % 4, (core + c) % 2

    def peer(offset):
        a, b, c = place(offset)
        return a * 8 + b * 2 + c

    barrier = pltpu.get_barrier_semaphore()
    partner = n + 1 - 2 * core

    def tell(north, deep):
        pl.semaphore_signal(barrier, inc=1, device_id=(north, deep), device_id_type=MESH)

    for offset in peer_order():
        a, b, _ = place(offset)
        if offset[2] == 0:
            tell(a * 8 + b * 2 + 1, d)
    for e in range(1, DEEP):
        tell(n - core, (d + e) % 4)
    tell(partner, d)

    def ready(first_core, count):
        @pl.when(core == first_core)
        def _():
            pl.semaphore_wait(barrier, count)
            pl.semaphore_signal(heard, inc=1, device_id=(partner, d), device_id_type=MESH)

        @pl.when(core != first_core)
        def _():
            pl.semaphore_wait(heard, 1)

    tabs = [
        pltpu.make_async_copy(a, b, tab_sem.at[i])
        for i, (a, b) in enumerate(
            [
                (x_hbm, x_tab),
                (y_hbm, y_tab),
                (fine_hbm, fine),
                (coarse_hbm, coarse),
                (sym_x_hbm, sym_x),
                (sym_y_hbm, sym_y),
                (sym_z_hbm, sym_z),
            ]
        )
    ]

    def load(y):
        return pltpu.make_async_copy(source.at[:, y, :], planes.at[y], load_sem.at[y])

    tabs[0].start()
    for y in range(16):
        load(y).start()
    for tab in tabs[1:]:
        tab.start()
    tabs[0].wait()

    flat_a = first_a.reshape(4 * 128 * 16, 128)

    def x_step(pair, _):
        for j in range(2):
            load(2 * pair + j).wait()
        for j in range(2):
            y = 2 * pair + j
            for half in range(2):
                high, low = split(planes[y, :, half * 256 : half * 256 + 256])
                res = dot3(x_tab[0], x_tab[1], high, low)
                for c in range(2):
                    cols = slice(c * 128, c * 128 + 128)
                    zc = half * 2 + c
                    for m in range(16):
                        row = (zc * 128 + m * 8) * 16
                        flat_a[pl.ds(row + y, 8, stride=16), :] = res[m * 8 : m * 8 + 8, cols]
                    first_b[zc, y] = res[128:, cols].reshape(4, 32, 128)
        return 0

    def send_first_b(q, _):
        for e in range(1, DEEP):
            to = (d + e) % 4
            pltpu.make_async_remote_copy(
                first_b.at[:, pl.ds(4 * q, 4), to],
                gath_b.at[q, d],
                y1_send,
                y1_recv.at[q],
                device_id=(n, to),
                device_id_type=MESH,
            ).start()
        return 0

    def send_first_a(half):
        def body(s, _):
            for offset in peer_order():
                to = peer(offset)
                pltpu.make_async_remote_copy(
                    first_a.at[s, pl.ds(4 * to, 4), pl.ds(8 * half, 8)],
                    gath_a.at[s, :, pl.ds(16 * n + 8 * half, 8)],
                    na_send,
                    na_recv.at[s],
                    device_id=(to, d),
                    device_id_type=MESH,
                ).start()
            return 0

        lax.fori_loop(0, 4, body, 0)

    def x_sends(q, _):
        send_first_b(q, 0)
        lax.fori_loop(2 * q + 2, 2 * q + 4, x_step, 0)
        return 0

    lax.fori_loop(0, 2, x_step, 0)
    ready(0, 2 * (DEEP - 1) + 1)
    lax.fori_loop(0, 2, x_sends, 0)
    send_first_b(2, 0)
    ready(1, NORTH - 1)
    send_first_a(0)
    lax.fori_loop(6, 8, x_step, 0)
    send_first_b(3, 0)
    send_first_a(1)

    for s in range(4):
        gath_a[s, :, pl.ds(16 * n, 16)] = first_a[s, pl.ds(4 * n, 4)]
        gath_b[s, d] = first_b[:, pl.ds(4 * s, 4), d]

    for tab in tabs[1:]:
        tab.wait()

    def table_step(p, _):
        for q in range(2):
            cols = slice(q * 512, q * 512 + 512)
            sin_p = coarse[0, pl.ds(p, 1), cols]
            cos_p = coarse[1, pl.ds(p, 1), cols]

            def rows_step(r, _):
                rows = pl.ds(pl.multiple_of(r * 16, 16), 16)
                values = sin_p * fine[1, rows, cols] + cos_p * fine[0, rows, cols]
                high, low = split(values)
                to = pl.ds(pl.multiple_of(p * 128 + r * 16, 16), 16)
                z_high[to, cols] = high
                z_low[to, cols] = low
                return 0

            lax.fori_loop(0, 8, rows_step, 0)
        return 0

    lax.fori_loop(0, 16, table_step, 0)

    row_id = lax.broadcasted_iota(jnp.int32, (128, 128), 0)
    col_id = lax.broadcasted_iota(jnp.int32, (128, 128), 1)
    for h in range(2):
        picked = jnp.where(row_id == col_id, sym_y[0:1, h * 128 : h * 128 + 128], 0.0)
        col_y[h * 128 : h * 128 + 128, :] = jnp.broadcast_to(
            jnp.sum(picked, axis=1, keepdims=True), (128, 128)
        )

    def z_stage(load_block, rows, store):
        for b in range(16):
            high, low = split(load_block(b))
            left_high[0:rows, b * 128 : b * 128 + 128] = high
            left_low[0:rows, b * 128 : b * 128 + 128] = low

        def col_step(t, _):
            cols = pl.ds(pl.multiple_of(t * 256, 256), 256)
            res = dot3(
                left_high[0:rows, :], left_low[0:rows, :], z_high[:, cols], z_low[:, cols]
            )
            store(t, cols, res)
            return 0

        lax.fori_loop(0, 4, col_step, 0)

    def step_a(s):
        wait_bytes(gath_a.at[s, :, pl.ds(0, 496)], na_recv.at[s])
        for i in range(0, 4, 2):
            high, low = split(jnp.concatenate([gath_a[s, i], gath_a[s, i + 1]], axis=1))
            res = dot3(y_tab[0], y_tab[1], high, low)
            half_a[s, i] = res[:, :128]
            half_a[s, i + 1] = res[:, 128:]
        for e in range(1, DEEP):
            to = (d + e) % 4
            pltpu.make_async_remote_copy(
                half_a.at[s, :, pl.ds(64 * to, 64)],
                recv_a.at[d, s],
                y2_send,
                y2_recv,
                device_id=(n, to),
                device_id_type=MESH,
            ).start()
        recv_a[d, s] = half_a[s, :, pl.ds(64 * d, 64)]

    flat_b = half_b.reshape(8 * 32 * 16, 128)

    def step_b(q):
        wait_bytes(gath_b.at[q, pl.ds(0, 3)], y1_recv.at[q])

        def store(t, cols, res):
            for c in range(2):
                for y in range(4):
                    for m in range(4):
                        at = y * 32 + m * 8
                        row = ((2 * t + c) * 32 + m * 8) * 16 + 4 * q + y
                        flat_b[pl.ds(row, 8, stride=16), :] = res[
                            at : at + 8, c * 128 : c * 128 + 128
                        ]

        z_stage(lambda b: gath_b[q, b // 4, b % 4].reshape(128, 128), 128, store)

    def send_half_b(modes, half, sem):
        for offset in peer_order():
            to = peer(offset)
            pltpu.make_async_remote_copy(
                half_b.at[modes, to, pl.ds(8 * half, 8)],
                recv_b.at[modes, pl.ds(16 * n + 8 * half, 8)],
                nb_send,
                sem,
                device_id=(to, d),
                device_id_type=MESH,
            ).start()

    def send_upper(ch, _):
        send_half_b(pl.ds(WIDE * ch, WIDE), 1, nb_recv.at[ch])
        return 0

    def middle_step(s, _):
        step_b(s)
        step_a(2 * s - 4)
        step_a(2 * s - 3)
        return 0

    lax.fori_loop(0, 2, lambda q, c: (step_b(q), c)[1], 0)
    send_half_b(slice(None), 0, nb_recv.at[CHUNKS])
    lax.fori_loop(2, 4, middle_step, 0)
    lax.fori_loop(0, CHUNKS, send_upper, 0)
    recv_b[:, pl.ds(16 * n, 16)] = half_b[:, n]
    wait_bytes(recv_b.at[:, pl.ds(0, 248)], nb_recv.at[CHUNKS])

    def last_step(ch, _):
        wait_bytes(recv_b.at[pl.ds(WIDE * ch, WIDE), pl.ds(0, 248)], nb_recv.at[ch])
        cols = pl.ds(pl.multiple_of(ch * WIDE * 128, WIDE * 128), WIDE * 128)
        high, low = split(jnp.concatenate([recv_b[WIDE * ch + j] for j in range(WIDE)], axis=1))
        res = dot3(y_tab[0], y_tab[1], high, low)
        symbol = (sym_x[8 * n + 4 + d] + col_y[:, 0:1]) + sym_z[0:1, cols]
        last_b[:, cols] = res * lax.rsqrt(symbol)
        for e in range(1, DEEP):
            to = (d + e) % 4
            pltpu.make_async_remote_copy(
                last_b.at[pl.ds(64 * to, 64), cols],
                out.at[4 + d, :, cols],
                y3_send,
                y3_recv,
                device_id=(n, to),
                device_id_type=MESH,
            ).start()
        out[4 + d, :, cols] = last_b[pl.ds(64 * d, 64), cols]
        return 0

    lax.fori_loop(0, CHUNKS, last_step, 0)

    wait_bytes(recv_a.at[pl.ds(0, 3)], y2_recv)

    def store_a(t, cols, res):
        for i in range(4):
            symbol = (sym_x[8 * n + i] + col_y[pl.ds(64 * d, 64), 0:1]) + sym_z[0:1, cols]
            out[i, :, cols] = res[i * 64 : i * 64 + 64] * lax.rsqrt(symbol)

    z_stage(lambda b: recv_a[b // 4, b % 4].reshape(256, 128), 256, store_a)

    wait_bytes(first_a.at[:, pl.ds(0, 124)], na_send)
    wait_bytes(gath_b.at[:, pl.ds(0, 3)], y1_send)
    wait_bytes(recv_a.at[pl.ds(0, 3)], y2_send)
    wait_bytes(half_b.at[:, pl.ds(0, 31)], nb_send)
    wait_bytes(last_b.at[pl.ds(0, 192)], y3_send)
    wait_bytes(last_b.at[pl.ds(0, 192)], y3_recv)


def halves(table):
    table = table.astype(np.float32)
    high = table.astype(BF16)
    return np.stack([high, (table - high.astype(np.float32)).astype(BF16)])


def tables():
    count = 512
    rank = np.arange(count, dtype=np.int64)
    angle = np.pi / (count + 1) * (((rank[:256, None] + 1) * (rank[None, :] + 1)) % (2 * count + 2))
    table = np.sin(angle) * np.sqrt(2.0 / (count + 1))
    rows = [8 * n + i for n in range(NORTH) for i in range(4)]
    rows += [8 * n + 4 + e for e in range(DEEP) for n in range(NORTH)]
    count = 2048
    rank = np.arange(1024, dtype=np.int64)[None, :] + 1
    step = np.pi / (count + 1)
    fine = step * ((np.arange(128, dtype=np.int64)[:, None] * rank) % (2 * count + 2))
    coarse = step * (((128 * np.arange(16, dtype=np.int64)[:, None] + 1) * rank) % (2 * count + 2))
    gain = np.sqrt(2.0 / (count + 1))
    fine = np.stack([np.sin(fine), np.cos(fine)]).astype(np.float32)
    coarse = (gain * np.stack([np.sin(coarse), np.cos(coarse)])).astype(np.float32)
    return halves(table[rows]), halves(table), fine, coarse


def on_device(source, symbol_x, symbol_y, symbol_z):
    vmem = pl.BlockSpec(memory_space=pltpu.VMEM)
    anywhere = pl.BlockSpec(memory_space=pl.ANY)
    dma = pltpu.SemaphoreType.DMA
    return pl.pallas_call(
        kernel,
        out_shape=pltpu.VMEM((8, 64, 1024), F32),
        in_specs=[anywhere] * 8,
        out_specs=vmem,
        scratch_shapes=[
            pltpu.VMEM((16, 512, 512), F32),
            pltpu.VMEM((2, 256, 512), BF16),
            pltpu.VMEM((2, 256, 512), BF16),
            pltpu.VMEM((2, 128, 1024), F32),
            pltpu.VMEM((2, 16, 1024), F32),
            pltpu.SMEM((512,), F32),
            pltpu.VMEM((1, 512), F32),
            pltpu.VMEM((1, 2048), F32),
            pltpu.VMEM((4, 128, 16, 128), F32),
            pltpu.VMEM((4, 16, 4, 32, 128), F32),
            pltpu.VMEM((4, 4, 512, 128), F32),
            pltpu.VMEM((4, 4, 4, 4, 32, 128), F32),
            pltpu.VMEM((4, 4, 256, 128), F32),
            pltpu.VMEM((4, 4, 4, 64, 128), F32),
            pltpu.VMEM((8, 32, 16, 128), F32),
            pltpu.VMEM((8, 512, 128), F32),
            pltpu.VMEM((256, 1024), F32),
            pltpu.VMEM((2048, 1024), BF16),
            pltpu.VMEM((2048, 1024), BF16),
            pltpu.VMEM((256, 2048), BF16),
            pltpu.VMEM((256, 2048), BF16),
            pltpu.VMEM((256, 128), F32),
            dma((16,)),
            dma((7,)),
            dma,
            dma((4,)),
            dma,
            dma((4,)),
            dma,
            dma,
            dma,
            dma((CHUNKS + 1,)),
            dma,
            dma,
            pltpu.SemaphoreType.REGULAR,
        ],
        compiler_params=pltpu.CompilerParams(
            collective_id=0, has_side_effects=True, vmem_limit_bytes=60 << 20
        ),
    )(
        source,
        *tables(),
        symbol_x,
        symbol_y.reshape(1, 512),
        symbol_z.reshape(1, 2048),
    )


def solution(mesh):
    in_specs = (P(None, "north", "deep"), P(), P(), P())
    out_specs = P("north", "deep", None)
    return jax.shard_map(
        on_device, mesh=mesh, in_specs=in_specs, out_specs=out_specs, check_vma=False
    )
```

```python
import functools

import jax
import jax.numpy as jnp
import numpy as np
from jax import lax
from jax.experimental import pallas as pl
from jax.experimental.pallas import tpu as pltpu
from jax.sharding import PartitionSpec as P

NORTH, DEEP = 32, 4
CHUNKS, WIDE = 8, 1
MESH = pl.DeviceIdType.MESH
F32, BF16 = jnp.float32, jnp.bfloat16


def split(values):
    high = values.astype(BF16)
    return high, (values - high.astype(F32)).astype(BF16)


def dot3(a_high, a_low, b_high, b_low):
    dot = functools.partial(jnp.dot, preferred_element_type=F32)
    return dot(a_high, b_high) + dot(a_low, b_high) + dot(a_high, b_low)


def peer_order():
    far = [0, 1, 2, 1]
    offsets = [(a, b, c) for a in range(4) for b in range(4) for c in range(2)]
    offsets.remove((0, 0, 0))
    return sorted(offsets, key=lambda o: (-(far[o[0]] + far[o[1]]), o[2], o[0], o[1]))


def wait_bytes(ref, sem):
    pltpu.make_async_copy(ref, ref, sem).wait()


def kernel(
    source, x_hbm, y_hbm, fine_hbm, coarse_hbm, sym_x_hbm, sym_y_hbm, sym_z_hbm, out,
    planes, x_tab, y_tab, fine, coarse, sym_x, sym_y, sym_z, first_a, first_b, gath_a, gath_b, half_a, recv_a,
    half_b, recv_b, last_b, z_high, z_low, left_high, left_low, col_y,
    load_sem, tab_sem, na_send, na_recv, y1_send, y1_recv, y2_send, y2_recv,
    nb_send, nb_recv, y3_send, y3_recv, heard,
):
    n = lax.axis_index("north")
    d = lax.axis_index("deep")
    z_pos, x_pos, core = n // 8, (n // 2) % 4, n % 2

    def place(offset):
        a, b, c = offset
        return (z_pos + a) % 4, (x_pos + b) % 4, (core + c) % 2

    def peer(offset):
        a, b, c = place(offset)
        return a * 8 + b * 2 + c

    barrier = pltpu.get_barrier_semaphore()
    partner = n + 1 - 2 * core

    def tell(north, deep):
        pl.semaphore_signal(barrier, inc=1, device_id=(north, deep), device_id_type=MESH)

    for offset in peer_order():
        a, b, _ = place(offset)
        if offset[2] == 0:
            tell(a * 8 + b * 2 + 1, d)
    for e in range(1, DEEP):
        tell(n - core, (d + e) % 4)
    tell(partner, d)

    def ready(first_core, count):
        @pl.when(core == first_core)
        def _():
            pl.semaphore_wait(barrier, count)
            pl.semaphore_signal(heard, inc=1, device_id=(partner, d), device_id_type=MESH)

        @pl.when(core != first_core)
        def _():
            pl.semaphore_wait(heard, 1)

    tabs = [
        pltpu.make_async_copy(a, b, tab_sem.at[i])
        for i, (a, b) in enumerate(
            [
                (x_hbm, x_tab),
                (y_hbm, y_tab),
                (fine_hbm, fine),
                (coarse_hbm, coarse),
                (sym_x_hbm, sym_x),
                (sym_y_hbm, sym_y),
                (sym_z_hbm, sym_z),
            ]
        )
    ]

    def load(y):
        return pltpu.make_async_copy(source.at[:, y, :], planes.at[y], load_sem.at[y])

    tabs[0].start()
    for y in range(16):
        load(y).start()
    for tab in tabs[1:]:
        tab.start()
    tabs[0].wait()

    flat_a = first_a.reshape(4 * 128 * 16, 128)

    def x_step(pair, _):
        for j in range(2):
            load(2 * pair + j).wait()
        for j in range(2):
            y = 2 * pair + j
            for half in range(2):
                high, low = split(planes[y, :, half * 256 : half * 256 + 256])
                res = dot3(x_tab[0], x_tab[1], high, low)
                for c in range(2):
                    cols = slice(c * 128, c * 128 + 128)
                    zc = half * 2 + c
                    for m in range(16):
                        row = (zc * 128 + m * 8) * 16
                        flat_a[pl.ds(row + y, 8, stride=16), :] = res[m * 8 : m * 8 + 8, cols]
                    first_b[zc, y] = res[128:, cols].reshape(4, 32, 128)
        return 0

    def send_first_b(q, _):
        for e in range(1, DEEP):
            to = (d + e) % 4
            pltpu.make_async_remote_copy(
                first_b.at[:, pl.ds(4 * q, 4), to],
                gath_b.at[q, d],
                y1_send,
                y1_recv.at[q],
                device_id=(n, to),
                device_id_type=MESH,
            ).start()
        return 0

    def send_first_a(half):
        def body(s, _):
            for offset in peer_order():
                to = peer(offset)
                pltpu.make_async_remote_copy(
                    first_a.at[s, pl.ds(4 * to, 4), pl.ds(8 * half, 8)],
                    gath_a.at[s, :, pl.ds(16 * n + 8 * half, 8)],
                    na_send,
                    na_recv.at[s],
                    device_id=(to, d),
                    device_id_type=MESH,
                ).start()
            return 0

        lax.fori_loop(0, 4, body, 0)

    def x_sends(q, _):
        send_first_b(q, 0)
        lax.fori_loop(2 * q + 2, 2 * q + 4, x_step, 0)
        return 0

    lax.fori_loop(0, 2, x_step, 0)
    ready(0, 2 * (DEEP - 1) + 1)
    lax.fori_loop(0, 1, x_sends, 0)
    send_first_b(1, 0)
    ready(1, NORTH - 1)
    send_first_a(0)
    lax.fori_loop(4, 6, x_step, 0)
    send_first_b(2, 0)
    lax.fori_loop(6, 8, x_step, 0)
    send_first_b(3, 0)
    send_first_a(1)

    for s in range(4):
        gath_a[s, :, pl.ds(16 * n, 16)] = first_a[s, pl.ds(4 * n, 4)]
        gath_b[s, d] = first_b[:, pl.ds(4 * s, 4), d]

    for tab in tabs[1:]:
        tab.wait()

    def table_step(p, _):
        for q in range(2):
            cols = slice(q * 512, q * 512 + 512)
            sin_p = coarse[0, pl.ds(p, 1), cols]
            cos_p = coarse[1, pl.ds(p, 1), cols]

            def rows_step(r, _):
                rows = pl.ds(pl.multiple_of(r * 16, 16), 16)
                values = sin_p * fine[1, rows, cols] + cos_p * fine[0, rows, cols]
                high, low = split(values)
                to = pl.ds(pl.multiple_of(p * 128 + r * 16, 16), 16)
                z_high[to, cols] = high
                z_low[to, cols] = low
                return 0

            lax.fori_loop(0, 8, rows_step, 0)
        return 0

    lax.fori_loop(0, 16, table_step, 0)

    row_id = lax.broadcasted_iota(jnp.int32, (128, 128), 0)
    col_id = lax.broadcasted_iota(jnp.int32, (128, 128), 1)
    for h in range(2):
        picked = jnp.where(row_id == col_id, sym_y[0:1, h * 128 : h * 128 + 128], 0.0)
        col_y[h * 128 : h * 128 + 128, :] = jnp.broadcast_to(
            jnp.sum(picked, axis=1, keepdims=True), (128, 128)
        )

    def z_stage(load_block, rows, store):
        for b in range(16):
            high, low = split(load_block(b))
            left_high[0:rows, b * 128 : b * 128 + 128] = high
            left_low[0:rows, b * 128 : b * 128 + 128] = low

        def col_step(t, _):
            cols = pl.ds(pl.multiple_of(t * 256, 256), 256)
            res = dot3(
                left_high[0:rows, :], left_low[0:rows, :], z_high[:, cols], z_low[:, cols]
            )
            store(t, cols, res)
            return 0

        lax.fori_loop(0, 4, col_step, 0)

    def step_a(s):
        wait_bytes(gath_a.at[s, :, pl.ds(0, 496)], na_recv.at[s])
        for i in range(0, 4, 2):
            high, low = split(jnp.concatenate([gath_a[s, i], gath_a[s, i + 1]], axis=1))
            res = dot3(y_tab[0], y_tab[1], high, low)
            half_a[s, i] = res[:, :128]
            half_a[s, i + 1] = res[:, 128:]
        for e in range(1, DEEP):
            to = (d + e) % 4
            pltpu.make_async_remote_copy(
                half_a.at[s, :, pl.ds(64 * to, 64)],
                recv_a.at[d, s],
                y2_send,
                y2_recv,
                device_id=(n, to),
                device_id_type=MESH,
            ).start()
        recv_a[d, s] = half_a[s, :, pl.ds(64 * d, 64)]

    flat_b = half_b.reshape(8 * 32 * 16, 128)

    def step_b(q):
        wait_bytes(gath_b.at[q, pl.ds(0, 3)], y1_recv.at[q])

        def store(t, cols, res):
            for c in range(2):
                for y in range(4):
                    for m in range(4):
                        at = y * 32 + m * 8
                        row = ((2 * t + c) * 32 + m * 8) * 16 + 4 * q + y
                        flat_b[pl.ds(row, 8, stride=16), :] = res[
                            at : at + 8, c * 128 : c * 128 + 128
                        ]

        z_stage(lambda b: gath_b[q, b // 4, b % 4].reshape(128, 128), 128, store)

    def send_half_b(modes, half, sem):
        for offset in peer_order():
            to = peer(offset)
            pltpu.make_async_remote_copy(
                half_b.at[modes, to, pl.ds(8 * half, 8)],
                recv_b.at[modes, pl.ds(16 * n + 8 * half, 8)],
                nb_send,
                sem,
                device_id=(to, d),
                device_id_type=MESH,
            ).start()

    def send_upper(ch, _):
        send_half_b(pl.ds(WIDE * ch, WIDE), 1, nb_recv.at[ch])
        return 0

    def middle_step(s, _):
        step_b(s)
        step_a(2 * s - 4)
        step_a(2 * s - 3)
        return 0

    lax.fori_loop(0, 2, lambda q, c: (step_b(q), c)[1], 0)
    send_half_b(pl.ds(0, 8), 0, nb_recv.at[CHUNKS])
    lax.fori_loop(2, 4, middle_step, 0)
    lax.fori_loop(0, CHUNKS, send_upper, 0)
    recv_b[:, pl.ds(16 * n, 16)] = half_b[:, n]
    wait_bytes(recv_b.at[:, pl.ds(0, 248)], nb_recv.at[CHUNKS])

    def last_step(ch, _):
        wait_bytes(recv_b.at[pl.ds(WIDE * ch, WIDE), pl.ds(0, 248)], nb_recv.at[ch])
        cols = pl.ds(pl.multiple_of(ch * WIDE * 128, WIDE * 128), WIDE * 128)
        high, low = split(jnp.concatenate([recv_b[WIDE * ch + j] for j in range(WIDE)], axis=1))
        res = dot3(y_tab[0], y_tab[1], high, low)
        symbol = (sym_x[8 * n + 4 + d] + col_y[:, 0:1]) + sym_z[0:1, cols]
        last_b[:, cols] = res * lax.rsqrt(symbol)
        for e in range(1, DEEP):
            to = (d + e) % 4
            pltpu.make_async_remote_copy(
                last_b.at[pl.ds(64 * to, 64), cols],
                out.at[4 + d, :, cols],
                y3_send,
                y3_recv,
                device_id=(n, to),
                device_id_type=MESH,
            ).start()
        out[4 + d, :, cols] = last_b[pl.ds(64 * d, 64), cols]
        return 0

    lax.fori_loop(0, CHUNKS, last_step, 0)

    wait_bytes(recv_a.at[pl.ds(0, 3)], y2_recv)

    def store_a(t, cols, res):
        for i in range(4):
            symbol = (sym_x[8 * n + i] + col_y[pl.ds(64 * d, 64), 0:1]) + sym_z[0:1, cols]
            out[i, :, cols] = res[i * 64 : i * 64 + 64] * lax.rsqrt(symbol)

    z_stage(lambda b: recv_a[b // 4, b % 4].reshape(256, 128), 256, store_a)

    wait_bytes(first_a.at[:, pl.ds(0, 124)], na_send)
    wait_bytes(gath_b.at[:, pl.ds(0, 3)], y1_send)
    wait_bytes(recv_a.at[pl.ds(0, 3)], y2_send)
    wait_bytes(half_b.at[:, pl.ds(0, 31)], nb_send)
    wait_bytes(last_b.at[pl.ds(0, 192)], y3_send)
    wait_bytes(last_b.at[pl.ds(0, 192)], y3_recv)


def halves(table):
    table = table.astype(np.float32)
    high = table.astype(BF16)
    return np.stack([high, (table - high.astype(np.float32)).astype(BF16)])


def tables():
    count = 512
    rank = np.arange(count, dtype=np.int64)
    angle = np.pi / (count + 1) * (((rank[:256, None] + 1) * (rank[None, :] + 1)) % (2 * count + 2))
    table = np.sin(angle) * np.sqrt(2.0 / (count + 1))
    rows = [8 * n + i for n in range(NORTH) for i in range(4)]
    rows += [8 * n + 4 + e for e in range(DEEP) for n in range(NORTH)]
    count = 2048
    rank = np.arange(1024, dtype=np.int64)[None, :] + 1
    step = np.pi / (count + 1)
    fine = step * ((np.arange(128, dtype=np.int64)[:, None] * rank) % (2 * count + 2))
    coarse = step * (((128 * np.arange(16, dtype=np.int64)[:, None] + 1) * rank) % (2 * count + 2))
    gain = np.sqrt(2.0 / (count + 1))
    fine = np.stack([np.sin(fine), np.cos(fine)]).astype(np.float32)
    coarse = (gain * np.stack([np.sin(coarse), np.cos(coarse)])).astype(np.float32)
    return halves(table[rows]), halves(table), fine, coarse


def on_device(source, symbol_x, symbol_y, symbol_z):
    vmem = pl.BlockSpec(memory_space=pltpu.VMEM)
    anywhere = pl.BlockSpec(memory_space=pl.ANY)
    dma = pltpu.SemaphoreType.DMA
    return pl.pallas_call(
        kernel,
        out_shape=pltpu.VMEM((8, 64, 1024), F32),
        in_specs=[anywhere] * 8,
        out_specs=vmem,
        scratch_shapes=[
            pltpu.VMEM((16, 512, 512), F32),
            pltpu.VMEM((2, 256, 512), BF16),
            pltpu.VMEM((2, 256, 512), BF16),
            pltpu.VMEM((2, 128, 1024), F32),
            pltpu.VMEM((2, 16, 1024), F32),
            pltpu.SMEM((512,), F32),
            pltpu.VMEM((1, 512), F32),
            pltpu.VMEM((1, 2048), F32),
            pltpu.VMEM((4, 128, 16, 128), F32),
            pltpu.VMEM((4, 16, 4, 32, 128), F32),
            pltpu.VMEM((4, 4, 512, 128), F32),
            pltpu.VMEM((4, 4, 4, 4, 32, 128), F32),
            pltpu.VMEM((4, 4, 256, 128), F32),
            pltpu.VMEM((4, 4, 4, 64, 128), F32),
            pltpu.VMEM((8, 32, 16, 128), F32),
            pltpu.VMEM((8, 512, 128), F32),
            pltpu.VMEM((256, 1024), F32),
            pltpu.VMEM((2048, 1024), BF16),
            pltpu.VMEM((2048, 1024), BF16),
            pltpu.VMEM((256, 2048), BF16),
            pltpu.VMEM((256, 2048), BF16),
            pltpu.VMEM((256, 128), F32),
            dma((16,)),
            dma((7,)),
            dma,
            dma((4,)),
            dma,
            dma((4,)),
            dma,
            dma,
            dma,
            dma((CHUNKS + 1,)),
            dma,
            dma,
            pltpu.SemaphoreType.REGULAR,
        ],
        compiler_params=pltpu.CompilerParams(
            collective_id=0, has_side_effects=True, vmem_limit_bytes=60 << 20
        ),
    )(
        source,
        *tables(),
        symbol_x,
        symbol_y.reshape(1, 512),
        symbol_z.reshape(1, 2048),
    )


def solution(mesh):
    in_specs = (P(None, "north", "deep"), P(), P(), P())
    out_specs = P("north", "deep", None)
    return jax.shard_map(
        on_device, mesh=mesh, in_specs=in_specs, out_specs=out_specs, check_vma=False
    )
```

```python
import functools

import jax
import jax.numpy as jnp
import numpy as np
from jax import lax
from jax.experimental import pallas as pl
from jax.experimental.pallas import tpu as pltpu
from jax.sharding import PartitionSpec as P

NORTH, DEEP = 32, 4
CHUNKS, WIDE = 8, 1
MESH = pl.DeviceIdType.MESH
F32, BF16 = jnp.float32, jnp.bfloat16


def split(values):
    high = values.astype(BF16)
    return high, (values - high.astype(F32)).astype(BF16)


def dot3(a_high, a_low, b_high, b_low):
    dot = functools.partial(jnp.dot, preferred_element_type=F32)
    return dot(a_high, b_high) + dot(a_low, b_high) + dot(a_high, b_low)


def peer_order():
    far = [0, 1, 2, 1]
    offsets = [(a, b, c) for a in range(4) for b in range(4) for c in range(2)]
    offsets.remove((0, 0, 0))
    return sorted(offsets, key=lambda o: (-(far[o[0]] + far[o[1]]), o[2], o[0], o[1]))


def wait_bytes(ref, sem):
    pltpu.make_async_copy(ref, ref, sem).wait()


def kernel(
    source, x_hbm, y_hbm, fine_hbm, coarse_hbm, sym_x_hbm, sym_y_hbm, sym_z_hbm, out,
    planes, x_tab, y_tab, fine, coarse, sym_x, sym_y, sym_z, first_a, first_b, gath_a, gath_b, half_a, recv_a,
    half_b, recv_b, last_b, z_high, z_low, left_high, left_low, col_y,
    load_sem, tab_sem, na_send, na_recv, y1_send, y1_recv, y2_send, y2_recv,
    nb_send, nb_recv, y3_send, y3_recv, heard,
):
    n = lax.axis_index("north")
    d = lax.axis_index("deep")
    z_pos, x_pos, core = n // 8, (n // 2) % 4, n % 2

    def place(offset):
        a, b, c = offset
        return (z_pos + a) % 4, (x_pos + b) % 4, (core + c) % 2

    def peer(offset):
        a, b, c = place(offset)
        return a * 8 + b * 2 + c

    barrier = pltpu.get_barrier_semaphore()
    partner = n + 1 - 2 * core

    def tell(north, deep):
        pl.semaphore_signal(barrier, inc=1, device_id=(north, deep), device_id_type=MESH)

    for offset in peer_order():
        a, b, _ = place(offset)
        if offset[2] == 0:
            tell(a * 8 + b * 2 + 1, d)
    for e in range(1, DEEP):
        tell(n - core, (d + e) % 4)
    tell(partner, d)

    def ready(first_core, count):
        @pl.when(core == first_core)
        def _():
            pl.semaphore_wait(barrier, count)
            pl.semaphore_signal(heard, inc=1, device_id=(partner, d), device_id_type=MESH)

        @pl.when(core != first_core)
        def _():
            pl.semaphore_wait(heard, 1)

    tabs = [
        pltpu.make_async_copy(a, b, tab_sem.at[i])
        for i, (a, b) in enumerate(
            [
                (x_hbm, x_tab),
                (y_hbm, y_tab),
                (fine_hbm, fine),
                (coarse_hbm, coarse),
                (sym_x_hbm, sym_x),
                (sym_y_hbm, sym_y),
                (sym_z_hbm, sym_z),
            ]
        )
    ]

    def load(y):
        return pltpu.make_async_copy(source.at[:, y, :], planes.at[y], load_sem.at[y])

    tabs[0].start()
    for y in range(16):
        load(y).start()
    for tab in tabs[1:]:
        tab.start()
    tabs[0].wait()

    flat_a = first_a.reshape(4 * 128 * 16, 128)

    def x_step(pair, _):
        for j in range(2):
            load(2 * pair + j).wait()
        for j in range(2):
            y = 2 * pair + j
            for half in range(2):
                high, low = split(planes[y, :, half * 256 : half * 256 + 256])
                res = dot3(x_tab[0], x_tab[1], high, low)
                for c in range(2):
                    cols = slice(c * 128, c * 128 + 128)
                    zc = half * 2 + c
                    for m in range(16):
                        row = (zc * 128 + m * 8) * 16
                        flat_a[pl.ds(row + y, 8, stride=16), :] = res[m * 8 : m * 8 + 8, cols]
                    first_b[zc, y] = res[128:, cols].reshape(4, 32, 128)
        return 0

    def send_first_b(q, _):
        for e in range(1, DEEP):
            to = (d + e) % 4
            pltpu.make_async_remote_copy(
                first_b.at[:, pl.ds(4 * q, 4), to],
                gath_b.at[q, d],
                y1_send,
                y1_recv.at[q],
                device_id=(n, to),
                device_id_type=MESH,
            ).start()
        return 0

    def send_first_a(half):
        def body(s, _):
            for offset in peer_order():
                to = peer(offset)
                pltpu.make_async_remote_copy(
                    first_a.at[s, pl.ds(4 * to, 4), pl.ds(8 * half, 8)],
                    gath_a.at[s, :, pl.ds(16 * n + 8 * half, 8)],
                    na_send,
                    na_recv.at[s],
                    device_id=(to, d),
                    device_id_type=MESH,
                ).start()
            return 0

        lax.fori_loop(0, 4, body, 0)

    def x_sends(q, _):
        send_first_b(q, 0)
        lax.fori_loop(2 * q + 2, 2 * q + 4, x_step, 0)
        return 0

    lax.fori_loop(0, 2, x_step, 0)
    ready(0, 2 * (DEEP - 1) + 1)
    lax.fori_loop(0, 1, x_sends, 0)
    send_first_b(1, 0)
    ready(1, NORTH - 1)
    send_first_a(0)
    lax.fori_loop(4, 6, x_step, 0)
    send_first_b(2, 0)
    lax.fori_loop(6, 8, x_step, 0)
    send_first_b(3, 0)
    send_first_a(1)

    for s in range(4):
        gath_a[s, :, pl.ds(16 * n, 16)] = first_a[s, pl.ds(4 * n, 4)]
        gath_b[s, d] = first_b[:, pl.ds(4 * s, 4), d]

    for tab in tabs[1:]:
        tab.wait()

    def table_step(p, _):
        for q in range(2):
            cols = slice(q * 512, q * 512 + 512)
            sin_p = coarse[0, pl.ds(p, 1), cols]
            cos_p = coarse[1, pl.ds(p, 1), cols]

            def rows_step(r, _):
                rows = pl.ds(pl.multiple_of(r * 16, 16), 16)
                values = sin_p * fine[1, rows, cols] + cos_p * fine[0, rows, cols]
                high, low = split(values)
                to = pl.ds(pl.multiple_of(p * 128 + r * 16, 16), 16)
                z_high[to, cols] = high
                z_low[to, cols] = low
                return 0

            lax.fori_loop(0, 8, rows_step, 0)
        return 0

    lax.fori_loop(0, 16, table_step, 0)

    row_id = lax.broadcasted_iota(jnp.int32, (128, 128), 0)
    col_id = lax.broadcasted_iota(jnp.int32, (128, 128), 1)
    for h in range(2):
        picked = jnp.where(row_id == col_id, sym_y[0:1, h * 128 : h * 128 + 128], 0.0)
        col_y[h * 128 : h * 128 + 128, :] = jnp.broadcast_to(
            jnp.sum(picked, axis=1, keepdims=True), (128, 128)
        )

    def z_left(load_block, rows):
        for b in range(16):
            high, low = split(load_block(b))
            left_high[0:rows, b * 128 : b * 128 + 128] = high
            left_low[0:rows, b * 128 : b * 128 + 128] = low

    def z_cols(rows, store, start, stop):
        def col_step(t, _):
            cols = pl.ds(pl.multiple_of(t * 256, 256), 256)
            res = dot3(
                left_high[0:rows, :], left_low[0:rows, :], z_high[:, cols], z_low[:, cols]
            )
            store(t, cols, res)
            return 0

        lax.fori_loop(start, stop, col_step, 0)

    def step_a(s):
        wait_bytes(gath_a.at[s, :, pl.ds(0, 496)], na_recv.at[s])
        for i in range(0, 4, 2):
            high, low = split(jnp.concatenate([gath_a[s, i], gath_a[s, i + 1]], axis=1))
            res = dot3(y_tab[0], y_tab[1], high, low)
            half_a[s, i] = res[:, :128]
            half_a[s, i + 1] = res[:, 128:]
        for e in range(1, DEEP):
            to = (d + e) % 4
            pltpu.make_async_remote_copy(
                half_a.at[s, :, pl.ds(64 * to, 64)],
                recv_a.at[d, s],
                y2_send,
                y2_recv,
                device_id=(n, to),
                device_id_type=MESH,
            ).start()
        recv_a[d, s] = half_a[s, :, pl.ds(64 * d, 64)]

    flat_b = half_b.reshape(8 * 32 * 16, 128)

    def step_b(q):
        wait_bytes(gath_b.at[q, pl.ds(0, 3)], y1_recv.at[q])

        def store(t, cols, res):
            for c in range(2):
                for y in range(4):
                    for m in range(4):
                        at = y * 32 + m * 8
                        row = ((2 * t + c) * 32 + m * 8) * 16 + 4 * q + y
                        flat_b[pl.ds(row, 8, stride=16), :] = res[
                            at : at + 8, c * 128 : c * 128 + 128
                        ]

        z_left(lambda b: gath_b[q, b // 4, b % 4].reshape(128, 128), 128)
        z_cols(128, store, 0, 4)

    def send_half_b(modes, half, sem):
        for offset in peer_order():
            to = peer(offset)
            pltpu.make_async_remote_copy(
                half_b.at[modes, to, pl.ds(8 * half, 8)],
                recv_b.at[modes, pl.ds(16 * n + 8 * half, 8)],
                nb_send,
                sem,
                device_id=(to, d),
                device_id_type=MESH,
            ).start()

    def send_upper(ch, _):
        send_half_b(pl.ds(WIDE * ch, WIDE), 1, nb_recv.at[ch])
        return 0

    def middle_step(s, _):
        step_b(s)
        step_a(2 * s - 4)
        step_a(2 * s - 3)
        return 0

    lax.fori_loop(0, 2, lambda q, c: (step_b(q), c)[1], 0)
    send_half_b(pl.ds(0, 8), 0, nb_recv.at[CHUNKS])
    lax.fori_loop(2, 3, middle_step, 0)
    step_b(3)
    lax.fori_loop(0, CHUNKS, send_upper, 0)
    lax.fori_loop(2, 4, lambda s, c: (step_a(s), c)[1], 0)
    recv_b[:, pl.ds(16 * n, 16)] = half_b[:, n]
    wait_bytes(recv_b.at[:, pl.ds(0, 248)], nb_recv.at[CHUNKS])

    def last_step(ch, _):
        wait_bytes(recv_b.at[pl.ds(WIDE * ch, WIDE), pl.ds(0, 248)], nb_recv.at[ch])
        cols = pl.ds(pl.multiple_of(ch * WIDE * 128, WIDE * 128), WIDE * 128)
        high, low = split(jnp.concatenate([recv_b[WIDE * ch + j] for j in range(WIDE)], axis=1))
        res = dot3(y_tab[0], y_tab[1], high, low)
        symbol = (sym_x[8 * n + 4 + d] + col_y[:, 0:1]) + sym_z[0:1, cols]
        last_b[:, cols] = res * lax.rsqrt(symbol)
        for e in range(1, DEEP):
            to = (d + e) % 4
            pltpu.make_async_remote_copy(
                last_b.at[pl.ds(64 * to, 64), cols],
                out.at[4 + d, :, cols],
                y3_send,
                y3_recv,
                device_id=(n, to),
                device_id_type=MESH,
            ).start()
        out[4 + d, :, cols] = last_b[pl.ds(64 * d, 64), cols]
        return 0

    def store_a(t, cols, res):
        for i in range(4):
            symbol = (sym_x[8 * n + i] + col_y[pl.ds(64 * d, 64), 0:1]) + sym_z[0:1, cols]
            out[i, :, cols] = res[i * 64 : i * 64 + 64] * lax.rsqrt(symbol)

    lax.fori_loop(0, 5, last_step, 0)
    wait_bytes(recv_a.at[pl.ds(0, 3)], y2_recv)
    z_left(lambda b: recv_a[b // 4, b % 4].reshape(256, 128), 256)
    z_cols(256, store_a, 0, 2)
    lax.fori_loop(5, CHUNKS, last_step, 0)
    z_cols(256, store_a, 2, 4)

    wait_bytes(first_a.at[:, pl.ds(0, 124)], na_send)
    wait_bytes(gath_b.at[:, pl.ds(0, 3)], y1_send)
    wait_bytes(recv_a.at[pl.ds(0, 3)], y2_send)
    wait_bytes(half_b.at[:, pl.ds(0, 31)], nb_send)
    wait_bytes(last_b.at[pl.ds(0, 192)], y3_send)
    wait_bytes(last_b.at[pl.ds(0, 192)], y3_recv)


def halves(table):
    table = table.astype(np.float32)
    high = table.astype(BF16)
    return np.stack([high, (table - high.astype(np.float32)).astype(BF16)])


def tables():
    count = 512
    rank = np.arange(count, dtype=np.int64)
    angle = np.pi / (count + 1) * (((rank[:256, None] + 1) * (rank[None, :] + 1)) % (2 * count + 2))
    table = np.sin(angle) * np.sqrt(2.0 / (count + 1))
    rows = [8 * n + i for n in range(NORTH) for i in range(4)]
    rows += [8 * n + 4 + e for e in range(DEEP) for n in range(NORTH)]
    count = 2048
    rank = np.arange(1024, dtype=np.int64)[None, :] + 1
    step = np.pi / (count + 1)
    fine = step * ((np.arange(128, dtype=np.int64)[:, None] * rank) % (2 * count + 2))
    coarse = step * (((128 * np.arange(16, dtype=np.int64)[:, None] + 1) * rank) % (2 * count + 2))
    gain = np.sqrt(2.0 / (count + 1))
    fine = np.stack([np.sin(fine), np.cos(fine)]).astype(np.float32)
    coarse = (gain * np.stack([np.sin(coarse), np.cos(coarse)])).astype(np.float32)
    return halves(table[rows]), halves(table), fine, coarse


def on_device(source, symbol_x, symbol_y, symbol_z):
    vmem = pl.BlockSpec(memory_space=pltpu.VMEM)
    anywhere = pl.BlockSpec(memory_space=pl.ANY)
    dma = pltpu.SemaphoreType.DMA
    return pl.pallas_call(
        kernel,
        out_shape=pltpu.VMEM((8, 64, 1024), F32),
        in_specs=[anywhere] * 8,
        out_specs=vmem,
        scratch_shapes=[
            pltpu.VMEM((16, 512, 512), F32),
            pltpu.VMEM((2, 256, 512), BF16),
            pltpu.VMEM((2, 256, 512), BF16),
            pltpu.VMEM((2, 128, 1024), F32),
            pltpu.VMEM((2, 16, 1024), F32),
            pltpu.SMEM((512,), F32),
            pltpu.VMEM((1, 512), F32),
            pltpu.VMEM((1, 2048), F32),
            pltpu.VMEM((4, 128, 16, 128), F32),
            pltpu.VMEM((4, 16, 4, 32, 128), F32),
            pltpu.VMEM((4, 4, 512, 128), F32),
            pltpu.VMEM((4, 4, 4, 4, 32, 128), F32),
            pltpu.VMEM((4, 4, 256, 128), F32),
            pltpu.VMEM((4, 4, 4, 64, 128), F32),
            pltpu.VMEM((8, 32, 16, 128), F32),
            pltpu.VMEM((8, 512, 128), F32),
            pltpu.VMEM((256, 1024), F32),
            pltpu.VMEM((2048, 1024), BF16),
            pltpu.VMEM((2048, 1024), BF16),
            pltpu.VMEM((256, 2048), BF16),
            pltpu.VMEM((256, 2048), BF16),
            pltpu.VMEM((256, 128), F32),
            dma((16,)),
            dma((7,)),
            dma,
            dma((4,)),
            dma,
            dma((4,)),
            dma,
            dma,
            dma,
            dma((CHUNKS + 1,)),
            dma,
            dma,
            pltpu.SemaphoreType.REGULAR,
        ],
        compiler_params=pltpu.CompilerParams(
            collective_id=0, has_side_effects=True, vmem_limit_bytes=60 << 20
        ),
    )(
        source,
        *tables(),
        symbol_x,
        symbol_y.reshape(1, 512),
        symbol_z.reshape(1, 2048),
    )


def solution(mesh):
    in_specs = (P(None, "north", "deep"), P(), P(), P())
    out_specs = P("north", "deep", None)
    return jax.shard_map(
        on_device, mesh=mesh, in_specs=in_specs, out_specs=out_specs, check_vma=False
    )
```
